512 devices in a mesh: depth: 256 (over z, y, x), chan: 2 (over core).
Axes of the slice: x: 4, y: 8, z: 8, core: 2. Of those that a mesh axis runs over, the one named last changes fastest.
Arguments:
- feats: bfloat16 [32, 512, 8, 128], P('chan', 'depth'), may hold values from -6 to 6
- weight_one: bfloat16 [32, 32, 27], replicated, may hold values from -0.21875 to 0.21875
- weight_two: bfloat16 [64, 32, 27], replicated, may hold values from -0.21875 to 0.21875
- cotangent: bfloat16 [64, 256, 4, 64], P('chan', 'depth'), may hold values from -6 to 6
Outputs:
- grad_feats: bfloat16 [32, 512, 8, 128], P('chan', 'depth')
- grad_weight_one: float32 [32, 32, 27], P(None, 'chan')
- grad_weight_two: float32 [64, 32, 27], P(None, 'chan')
The draws below stay inside these ranges and needn't reach their ends.
All inputs are finite; a program needn't handle non-finite values.
Results may differ from the reference program's by a relative error of at most 0.013.
Values may be sent and summed in bfloat16 or wider, within the bound.
A program may use at most 128 MiB of HBM per device.

```python
import jax
import jax.numpy as jnp
from jax import lax

C0 = 32
C1 = 64
H = 8
W = 128
NZ = 512


def shard_levels(rng, dims, cuts, low, largest):
    factor_of, own = 1.0, jax.random.fold_in(rng, 6)
    for axis_at, blocks in cuts:
        draws = jnp.exp(jax.random.uniform(jax.random.fold_in(own, axis_at), (blocks,), jnp.float32, low / len(cuts), largest / len(cuts)))
        factor_of = factor_of * jnp.repeat(draws, dims[axis_at] // blocks).reshape([-1 if axis == axis_at else 1 for axis in range(len(dims))])
    return factor_of


def gaussian(rng, shape, scale, bound, cuts=(), held_as=jnp.bfloat16):
    entries = scale * jax.random.normal(rng, shape, jnp.float32)
    if cuts:
        entries = entries * shard_levels(rng, shape, cuts, -0.22, 0.18)
    return jnp.clip(entries, -bound, bound).astype(held_as)


def setup_inputs(seed: int = 0) -> dict:
    splits = jax.random.split(jax.random.key(seed), 5)
    feats = gaussian(splits[0], (C0, NZ, H, W), 1.0, 6.0, ((0, 2), (1, 256)))
    weight_one = gaussian(splits[1], (C0, C0, 27), (27 * C0) ** -0.5, 0.21875)
    weight_two = gaussian(splits[2], (C1, C0, 27), (27 * C0) ** -0.5, 0.21875)
    cotangent = gaussian(splits[3], (C1, NZ // 2, H // 2, W // 2), 1.0, 6.0, ((0, 2), (1, 256)))
    return dict(feats=feats, weight_one=weight_one, weight_two=weight_two, cotangent=cotangent)


OFFSETS = [(first, second, third) for first in range(3) for second in range(3) for third in range(3)]

def pad_all(field):
    return jnp.pad(field.astype(jnp.float32), ((0, 0), (1, 1), (1, 1), (1, 1)))

def convolve(field, weight):
    chans, planes, height, across = field.shape
    padded = pad_all(field)
    total = jnp.zeros((weight.shape[0], planes, height, across), jnp.float32)
    for index, (first, second, third) in enumerate(OFFSETS):
        window = padded[:, first:first + planes, second:second + height, third:third + across]
        total = total + jnp.einsum('oi,izhw->ozhw', weight[:, :, index].astype(jnp.float32), window, precision=lax.Precision.HIGHEST)
    return total

def transpose_conv(grads, weight):
    chans, planes, height, across = grads.shape
    padded = pad_all(grads)
    total = jnp.zeros((weight.shape[1], planes, height, across), jnp.float32)
    for index, (first, second, third) in enumerate(OFFSETS):
        window = padded[:, 2 - first:2 - first + planes, 2 - second:2 - second + height, 2 - third:2 - third + across]
        total = total + jnp.einsum('oi,ozhw->izhw', weight[:, :, index].astype(jnp.float32), window, precision=lax.Precision.HIGHEST)
    return total

def weight_grad(grads, field):
    chans, planes, height, across = field.shape
    padded = pad_all(field)
    grads_wide = grads.astype(jnp.float32)
    pieces = []
    for index, (first, second, third) in enumerate(OFFSETS):
        window = padded[:, first:first + planes, second:second + height, third:third + across]
        pieces.append(jnp.einsum('ozhw,izhw->oi', grads_wide, window, precision=lax.Precision.HIGHEST))
    return jnp.stack(pieces, axis=-1)

def slope(pre):
    sig = jax.nn.sigmoid(pre)
    return sig * (1.0 + pre * (1.0 - sig))

def one_volume(feats, weight_one, weight_two, cotangent):
    chans, planes, height, across = feats.shape
    pre_one = convolve(feats, weight_one)
    act_one = jax.nn.silu(pre_one).astype(jnp.bfloat16)
    pooled = act_one.astype(jnp.float32).reshape(chans, planes // 2, 2, height // 2, 2, across // 2, 2).mean(axis=(2, 4, 6)).astype(jnp.bfloat16)
    pre_two = convolve(pooled, weight_two)
    grad_two = (cotangent.astype(jnp.float32) * slope(pre_two)).astype(jnp.bfloat16)
    grad_weight_two = weight_grad(grad_two, pooled)
    back_pooled = transpose_conv(grad_two, weight_two)
    spread = jnp.repeat(jnp.repeat(jnp.repeat(back_pooled, 2, axis=1), 2, axis=2), 2, axis=3) * 0.125
    grad_one = (spread * slope(pre_one)).astype(jnp.bfloat16)
    grad_weight_one = weight_grad(grad_one, feats)
    grad_feats = transpose_conv(grad_one, weight_one).astype(jnp.bfloat16)
    return (grad_feats, grad_weight_one, grad_weight_two)

def reference(feats, weight_one, weight_two, cotangent):
    return one_volume(feats, weight_one, weight_two, cotangent)
```

```python
import functools

import jax
import jax.numpy as jnp
from jax import lax
from jax.experimental import pallas as pl
from jax.experimental.pallas import tpu as pltpu
from jax.sharding import Mesh
from jax.sharding import PartitionSpec as P

MESH = pl.DeviceIdType.MESH
F32 = jnp.float32
BF16 = jnp.bfloat16
AXES = ("z", "y", "x", "core")
ROWS = 512


def slope_of(pre, sig):
    return sig * (1.0 + pre * (1.0 - sig))


def fill_columns(dst, plane, chans, row, value, edges):
    lane = lax.broadcasted_iota(jnp.int32, value.shape, 1)
    left = pltpu.roll(value, 1, 1)
    right = pltpu.roll(value, 127, 1)
    if edges:
        left = jnp.where(lane == 0, 0.0, left)
        right = jnp.where(lane == 127, 0.0, right)
    where = slice((row + 1) * 128, (row + 2) * 128)
    dst[plane, 0:chans, where] = left.astype(BF16)
    dst[plane, chans : 2 * chans, where] = value.astype(BF16)
    dst[plane, 2 * chans : 3 * chans, where] = right.astype(BF16)


def clear_rows(dst, rows):
    planes, chans = dst.shape[:2]
    zero = jnp.zeros((planes, chans, 128), BF16)
    dst[:, :, 0:128] = zero
    dst[:, :, (rows + 1) * 128 : (rows + 2) * 128] = zero


def windows(src, planes, width):
    pieces = [src[a, :, b * 128 : b * 128 + width] for a in planes for b in range(3)]
    return jnp.concatenate(pieces, axis=0)


def own_windows(src, planes, width, core):
    pieces = []
    for a in planes:
        for b in range(3):
            for c in range(3):
                first = pl.multiple_of(c * 32 + core * 16, 16)
                pieces.append(src[a, pl.ds(first, 16), b * 128 : b * 128 + width])
    return jnp.concatenate(pieces, axis=0)


def pack_rows(rows):
    return jnp.concatenate(
        [rows[0] + pltpu.roll(rows[2], 64, 1), rows[1] + pltpu.roll(rows[3], 64, 1)], axis=1
    )


def unpack_into(dst, plane, chans, packed):
    lane = lax.broadcasted_iota(jnp.int32, (chans, 128), 1)
    for j in range(2):
        both = packed[:, j * 128 : (j + 1) * 128]
        low = jnp.where(lane < 64, both, 0.0)
        high = jnp.where(lane < 64, pltpu.roll(both, 64, 1), 0.0)
        fill_columns(dst, plane, chans, j, low, False)
        fill_columns(dst, plane, chans, j + 2, high, False)


def kernel(
    sizes,
    feats,
    w1f,
    w2f,
    w2b,
    w1b,
    cot,
    gf,
    gw1,
    gw2,
    fr,
    turn,
    x1,
    s1,
    p2r,
    x2,
    g2r,
    g2c,
    g1r,
    g1c,
    ws,
    rx,
    acc1,
    ry,
    acc2,
    rz,
    fin,
    send,
    recv,
):
    nz, ny, nx = sizes
    z, y, x, core = (lax.axis_index(a) for a in AXES)
    total = nz * ny * nx
    place = (z * ny + y) * nx + x

    def at(position, c):
        return (position // (nx * ny), (position // nx) % ny, position % nx, c)

    left = (place + total - 1) % total
    right = (place + 1) % total
    other = 1 - core
    near = [
        (z, y, x, other),
        at(left, core),
        at(left, other),
        at(right, core),
        at(right, other),
    ]
    along_x = [(z, y, (x + k) % nx, core) for k in range(1, nx)]
    along_y = [(z, (y + k) % ny, x, core) for k in range(1, ny)]
    along_z = [((z + k) % nz, y, x, core) for k in range(1, nz)]

    barrier = pltpu.get_barrier_semaphore()
    peers = near + along_x + along_y + along_z
    for peer in peers:
        pl.semaphore_signal(barrier, inc=1, device_id=peer, device_id_type=MESH)
    pl.semaphore_wait(barrier, len(peers))

    count = [0]

    def copy(src, dst, peer):
        k = count[0]
        count[0] += 1
        made = pltpu.make_async_remote_copy(
            src_ref=src,
            dst_ref=dst,
            send_sem=send.at[k],
            recv_sem=recv.at[k],
            device_id=peer,
            device_id_type=MESH,
        )
        made.start()
        return made

    started = []
    half = pl.ds(pl.multiple_of(core * 16, 16), 16)
    half2 = pl.ds(pl.multiple_of(core * 32, 32), 32)

    batch = [
        copy(feats.at[:, 0], fr.at[3, half], near[1]),
        copy(feats.at[:, 0], fr.at[3, half], near[2]),
        copy(feats.at[:, 1], fr.at[0, half], near[3]),
        copy(feats.at[:, 1], fr.at[0, half], near[4]),
        copy(feats.at[:, 0], fr.at[1, half], near[0]),
        copy(feats.at[:, 1], fr.at[2, half], near[0]),
    ]
    started += batch
    fr[1, half] = feats[:, 0]
    fr[2, half] = feats[:, 1]
    clear_rows(x1, 8)
    clear_rows(x2, 4)
    clear_rows(g2c, 4)
    clear_rows(g1c, 8)
    for c in range(32):
        turn[4, c * 8 : c * 8 + 4, 0:64] = cot[c, 0].astype(F32)
    lane = lax.broadcasted_iota(jnp.int32, (32, 128), 1)
    cots = [
        jnp.where(lane < 64, turn[4, pl.ds(r, 32, stride=8), :], 0.0) for r in range(4)
    ]
    cots = jnp.concatenate(cots, axis=1)
    lower = place > 0
    upper = place < total - 1
    for made in batch[::-1]:
        made.wait_recv()
    for p in (1, 2, 0, 3):
        turn[p] = fr[p].astype(F32).reshape(256, 128)
        for r in range(8):
            value = turn[p, pl.ds(r, 32, stride=8), :]
            if p == 0:
                value = jnp.where(lower, value, 0.0)
            if p == 3:
                value = jnp.where(upper, value, 0.0)
            fill_columns(x1, p, 32, r, value, True)

    own_w1f = w1f[half, :]
    act = []
    for plane in range(2):
        pre = jnp.dot(
            own_w1f, windows(x1, range(plane, plane + 3), 1024), preferred_element_type=F32
        )
        sig = jax.nn.sigmoid(pre)
        s1[:, plane * 1024 : (plane + 1) * 1024] = slope_of(pre, sig)
        act.append((pre * sig).astype(BF16))

    def act_row(plane, r):
        return act[plane][:, r * 128 : (r + 1) * 128]

    spots = jnp.concatenate(
        [
            jnp.concatenate(
                [act_row(a, 2 * r + b) for a in range(2) for b in range(2)], axis=1
            )
            for r in range(4)
        ],
        axis=0,
    )
    from_cell = lax.broadcasted_iota(jnp.int32, (512, 128), 0)
    to_cell = lax.broadcasted_iota(jnp.int32, (512, 128), 1)
    pool = jnp.where(((from_cell & 127) >> 1) == to_cell, 0.125, 0.0).astype(BF16)
    pooled = jnp.dot(spots, pool, preferred_element_type=F32)
    pooled = pooled.astype(BF16).astype(F32)
    p2r[1, half] = pack_rows([pooled[16 * r : 16 * r + 16] for r in range(4)]).astype(BF16)

    def exchange(ref, part):
        return [
            copy(ref.at[1, part], ref.at[2, part], near[1]),
            copy(ref.at[1, part], ref.at[2, part], near[2]),
            copy(ref.at[1, part], ref.at[0, part], near[3]),
            copy(ref.at[1, part], ref.at[0, part], near[4]),
            copy(ref.at[1, part], ref.at[1, part], near[0]),
        ]

    batch = exchange(p2r, half)
    started += batch
    for made in batch[::-1]:
        made.wait_recv()
    for p in range(3):
        packed = p2r[p].astype(F32)
        if p == 0:
            packed = jnp.where(lower, packed, 0.0)
        if p == 2:
            packed = jnp.where(upper, packed, 0.0)
        unpack_into(x2, p, 32, packed)

    pre = jnp.dot(w2f[half2, :], windows(x2, range(3), 512), preferred_element_type=F32)
    sig = jax.nn.sigmoid(pre)
    grad = cots * slope_of(pre, sig)
    grad = grad.astype(BF16).astype(F32)
    g2r[1, half2] = pack_rows([grad[:, r * 128 : (r + 1) * 128] for r in range(4)]).astype(BF16)
    batch = exchange(g2r, half2)
    started += batch
    for made in batch[::-1]:
        made.wait_recv()
    for p in range(3):
        packed = g2r[p].astype(F32)
        if p == 0:
            packed = jnp.where(lower, packed, 0.0)
        if p == 2:
            packed = jnp.where(upper, packed, 0.0)
        unpack_into(g2c, p, 64, packed)

    back = jnp.dot(w2b[half, :], windows(g2c, range(3), 512), preferred_element_type=F32)
    back = jnp.concatenate([back[:, r * 128 : (r + 1) * 128] for r in range(4)], axis=0)
    high = back.astype(BF16)
    rest = back - high.astype(F32)
    middle = rest.astype(BF16)
    low = (rest - middle.astype(F32)).astype(BF16)
    from_cell = lax.broadcasted_iota(jnp.int32, (128, 128), 0)
    to_cell = lax.broadcasted_iota(jnp.int32, (128, 128), 1)
    spread = jnp.where(from_cell == (to_cell >> 1), 1.0, 0.0).astype(BF16)
    wide = jnp.dot(
        jnp.concatenate([high, middle, low], axis=0), spread, preferred_element_type=F32
    )
    wide = (wide[0:64] + wide[64:128] + wide[128:192]) * 0.125
    for plane in range(2):
        for r in range(8):
            first = plane * 1024 + r * 128
            value = wide[(r // 2) * 16 : (r // 2) * 16 + 16] * s1[:, first : first + 128]
            g1r[1 + plane, half, r * 128 : (r + 1) * 128] = value.astype(BF16)
    both = pl.ds(1, 2)
    batch = [
        copy(g1r.at[both, half], g1r.at[both, half], near[0]),
        copy(g1r.at[1, half], g1r.at[3, half], near[1]),
        copy(g1r.at[1, half], g1r.at[3, half], near[2]),
        copy(g1r.at[2, half], g1r.at[0, half], near[3]),
        copy(g1r.at[2, half], g1r.at[0, half], near[4]),
    ]
    started += batch

    nothing = jnp.zeros((64, 512), BF16)
    contract = (((1,), (1,)), ((), ()))
    sums = lax.dot_general(
        own_windows(x2, range(3), 512, core),
        jnp.concatenate([g2c[1, 64:128, 128:640], nothing], axis=0),
        contract,
        preferred_element_type=F32,
    )

    def fill_grad(p):
        for r in range(8):
            value = g1r[p, :, r * 128 : (r + 1) * 128].astype(F32)
            if p == 0:
                value = jnp.where(lower, value, 0.0)
            if p == 3:
                value = jnp.where(upper, value, 0.0)
            fill_columns(g1c, p, 32, r, value, True)

    batch[0].wait_recv()
    fill_grad(1)
    fill_grad(2)
    for plane in range(2):
        sums += lax.dot_general(
            own_windows(x1, range(plane, plane + 3), 1024, core),
            jnp.concatenate(
                [
                    jnp.zeros((64, 1024), BF16),
                    g1c[1 + plane, 32:64, 128:1152],
                    jnp.zeros((32, 1024), BF16),
                ],
                axis=0,
            ),
            contract,
            preferred_element_type=F32,
        )
    ws[0:432] = sums
    ws[432:ROWS] = jnp.zeros((ROWS - 432, 128), F32)

    part_x = ROWS // nx
    part_y = part_x // ny

    def rows_x(i):
        return pl.ds(pl.multiple_of(i * part_x, part_x), part_x)

    def rows_y(i):
        return pl.ds(pl.multiple_of(i * part_y, part_y), part_y)

    batch_x = [copy(ws.at[rows_x(peer[2])], rx.at[x], peer) for peer in along_x]
    started += batch_x

    for made in batch[1:]:
        made.wait_recv()
    fill_grad(0)
    fill_grad(3)
    own_w1b = w1b[half, :]
    for plane in range(2):
        grad = jnp.dot(
            own_w1b, windows(g1c, range(plane, plane + 3), 1024), preferred_element_type=F32
        )
        for r in range(8):
            turn[plane, pl.ds(r, 16, stride=8), :] = grad[:, r * 128 : (r + 1) * 128]
        gf[:, plane] = turn[plane, 0:128].reshape(16, 8, 128).astype(BF16)

    for made in batch_x:
        made.wait_recv()
    sums = ws[rows_x(x)]
    for k in range(1, nx):
        sums += rx[(x + k) % nx]
    acc1[...] = sums
    batch = [copy(acc1.at[rows_y(peer[1])], ry.at[y], peer) for peer in along_y]
    started += batch
    for made in batch:
        made.wait_recv()
    sums = acc1[rows_y(y)]
    for k in range(1, ny):
        sums += ry[(y + k) % ny]
    acc2[...] = sums
    rz[z] = sums
    batch = [copy(acc2, rz.at[z], peer) for peer in along_z]
    started += batch
    for made in batch:
        made.wait_recv()
    sums = rz[0]
    for k in range(1, nz):
        sums += rz[k]
    mine = pl.ds(pl.multiple_of(x * part_x + y * part_y, part_y), part_y)
    fin[mine] = sums
    batch = [copy(fin.at[mine], fin.at[mine], peer) for peer in along_y]
    started += batch
    for made in batch:
        made.wait_recv()
    batch = [copy(fin.at[rows_x(x)], fin.at[rows_x(x)], peer) for peer in along_x]
    started += batch
    for made in batch:
        made.wait_recv()
    gw2[...] = fin[0:432, 0:64]
    gw1[...] = pltpu.roll(fin[0:432], 64, 1)[:, 0:32]
    for made in started:
        made.wait_send()


def shards(sizes, feats, weight_one, weight_two, cotangent):
    nz, ny, nx = sizes
    w1f = jnp.transpose(weight_one, (0, 2, 1)).reshape(32, 27 * 32)
    w2f = jnp.transpose(weight_two, (0, 2, 1)).reshape(64, 27 * 32)
    w2b = jnp.transpose(weight_two[:, :, ::-1], (1, 2, 0)).reshape(32, 27 * 64)
    w1b = jnp.transpose(weight_one[:, :, ::-1], (1, 2, 0)).reshape(32, 27 * 32)
    copies = 6 + 5 + 5 + 5 + 2 * (nx - 1) + 2 * (ny - 1) + (nz - 1)
    part_x = ROWS // nx
    part_y = part_x // ny
    vmem = pl.BlockSpec(memory_space=pltpu.VMEM)
    gf, gw1, gw2 = pl.pallas_call(
        functools.partial(kernel, sizes),
        out_shape=(
            jax.ShapeDtypeStruct((16, 2, 8, 128), BF16),
            jax.ShapeDtypeStruct((432, 32), F32),
            jax.ShapeDtypeStruct((432, 64), F32),
        ),
        in_specs=[vmem] * 6,
        out_specs=(vmem, vmem, vmem),
        scratch_shapes=[
            pltpu.VMEM((4, 32, 8, 128), BF16),
            pltpu.VMEM((5, 256, 128), F32),
            pltpu.VMEM((4, 96, 1280), BF16),
            pltpu.VMEM((16, 2048), F32),
            pltpu.VMEM((3, 32, 256), BF16),
            pltpu.VMEM((3, 96, 768), BF16),
            pltpu.VMEM((3, 64, 256), BF16),
            pltpu.VMEM((3, 192, 768), BF16),
            pltpu.VMEM((4, 32, 1024), BF16),
            pltpu.VMEM((4, 96, 1280), BF16),
            pltpu.VMEM((ROWS, 128), F32),
            pltpu.VMEM((nx, part_x, 128), F32),
            pltpu.VMEM((part_x, 128), F32),
            pltpu.VMEM((ny, part_y, 128), F32),
            pltpu.VMEM((part_y, 128), F32),
            pltpu.VMEM((nz, part_y, 128), F32),
            pltpu.VMEM((ROWS, 128), F32),
            pltpu.SemaphoreType.DMA((copies,)),
            pltpu.SemaphoreType.DMA((copies,)),
        ],
        compiler_params=pltpu.CompilerParams(collective_id=0, has_side_effects=True),
    )(feats, w1f, w2f, w2b, w1b, cotangent)
    gw1 = jnp.transpose(gw1.reshape(27, 16, 32), (2, 1, 0))
    gw2 = jnp.transpose(gw2.reshape(27, 16, 64), (2, 1, 0))
    return gf, gw1, gw2


def build(mesh, sizes):
    finer = Mesh(mesh.devices.reshape(*sizes, mesh.shape["chan"]), AXES)
    depth = AXES[:3]
    in_specs = (P("core", depth, None, None), P(), P(), P("core", depth, None, None))
    out_specs = (P("core", depth, None, None), P(None, "core", None), P(None, "core", None))
    return jax.shard_map(
        functools.partial(shards, sizes),
        mesh=finer,
        in_specs=in_specs,
        out_specs=out_specs,
        check_vma=False,
    )


def solution(mesh):
    return build(mesh, (8, 8, 4))
```

```python
import functools

import jax
import jax.numpy as jnp
from jax import lax
from jax.experimental import pallas as pl
from jax.experimental.pallas import tpu as pltpu
from jax.sharding import Mesh
from jax.sharding import PartitionSpec as P

MESH = pl.DeviceIdType.MESH
F32 = jnp.float32
BF16 = jnp.bfloat16
AXES = ("z", "y", "x", "core")


def slope_of(pre, sig):
    return sig * (1.0 + pre * (1.0 - sig))


def fill_columns(dst, plane, chans, row, value, edges, flip):
    lane = lax.broadcasted_iota(jnp.int32, value.shape, 1)
    before = pltpu.roll(value, 1, 1)
    after = pltpu.roll(value, 127, 1)
    if edges:
        before = jnp.where(lane == 0, 0.0, before)
        after = jnp.where(lane == 127, 0.0, after)
    where = slice((row + 1) * 128, (row + 2) * 128)
    first, last = (after, before) if flip else (before, after)
    dst[plane, 0:chans, where] = first.astype(BF16)
    dst[plane, chans : 2 * chans, where] = value.astype(BF16)
    dst[plane, 2 * chans : 3 * chans, where] = last.astype(BF16)


def clear_rows(dst, rows):
    planes, chans = dst.shape[:2]
    zero = jnp.zeros((planes, chans, 128), BF16)
    dst[:, :, 0:128] = zero
    dst[:, :, (rows + 1) * 128 : (rows + 2) * 128] = zero


def windows(src, plane, width, flip=False):
    order = (2, 1, 0) if flip else (0, 1, 2)
    return jnp.concatenate([src[plane, :, b * 128 : b * 128 + width] for b in order], axis=0)


def own_windows(src, planes, width, core):
    pieces = []
    for a in planes:
        for b in range(3):
            for c in range(3):
                first = pl.multiple_of(c * 32 + core * 16, 16)
                pieces.append(src[a, pl.ds(first, 16), b * 128 : b * 128 + width])
    return jnp.concatenate(pieces, axis=0)


def pack_rows(rows):
    return jnp.concatenate(
        [rows[0] + pltpu.roll(rows[2], 64, 1), rows[1] + pltpu.roll(rows[3], 64, 1)], axis=1
    )


def unpack_into(dst, plane, chans, packed, flip):
    lane = lax.broadcasted_iota(jnp.int32, (chans, 128), 1)
    for j in range(2):
        both = packed[:, j * 128 : (j + 1) * 128]
        low = jnp.where(lane < 64, both, 0.0)
        high = jnp.where(lane < 64, pltpu.roll(both, 64, 1), 0.0)
        fill_columns(dst, plane, chans, j, low, False, flip)
        fill_columns(dst, plane, chans, j + 2, high, False, flip)


def dot(a, b):
    return jnp.dot(a, b, preferred_element_type=F32)


def dot_rows(a, b):
    return lax.dot_general(a, b, (((1,), (1,)), ((), ())), preferred_element_type=F32)


def kernel(
    sizes,
    feats,
    weight_one,
    weight_two,
    cotangent,
    gf,
    out1,
    out2,
    w1,
    w2,
    cot,
    w1f,
    w2f,
    w2b,
    w1b,
    turned,
    fr,
    turn,
    x1,
    s1,
    p2r,
    x2,
    g2r,
    g2c,
    g1r,
    g1c,
    gfv,
    ws1,
    rx1,
    acc1,
    rz1,
    fin1,
    ws2,
    rx2,
    acc2,
    rz2,
    fin2,
    local,
    send,
    recv,
    sum_send,
    sum_recv,
):
    nz, ny, nx = sizes
    z, y, x, core = (lax.axis_index(a) for a in AXES)
    total = nz * ny * nx
    place = (z * ny + y) * nx + x
    flat = nx * ny
    half = pl.ds(pl.multiple_of(core * 16, 16), 16)
    half2 = pl.ds(pl.multiple_of(core * 32, 32), 32)

    def fetch(src, dst, k):
        made = pltpu.make_async_copy(src, dst, local.at[k])
        made.start()
        return made

    fetched = [
        fetch(feats.at[:, 0], fr.at[1, half], 0),
        fetch(feats.at[:, 1], fr.at[2, half], 1),
        fetch(weight_one, w1, 2),
        fetch(weight_two, w2, 3),
        fetch(cotangent, cot, 4),
    ]

    def at(position, c):
        return (position // (nx * ny), (position // nx) % ny, position % nx, c)

    left = (place + total - 1) % total
    right = (place + 1) % total
    other = 1 - core
    near = [
        (z, y, x, other),
        at(left, core),
        at(left, other),
        at(right, core),
        at(right, other),
    ]
    steps = [(i, j) for i in range(ny) for j in range(nx) if i or j]
    steps.sort(key=lambda s: -(min(s[0], ny - s[0]) + min(s[1], nx - s[1])))
    across = [(z, (y + i) % ny, (x + j) % nx, core) for i, j in steps]
    along_z = [((z + k) % nz, y, x, core) for k in range(1, nz)]
    mine = y * nx + x

    barrier = pltpu.get_barrier_semaphore()
    peers = near + across + along_z
    for peer in peers:
        pl.semaphore_signal(barrier, inc=1, device_id=peer, device_id_type=MESH)
    pl.semaphore_wait(barrier, len(peers))

    count = [0]
    started = []

    def copy(src, dst, peer):
        k = count[0]
        count[0] += 1
        made = pltpu.make_async_remote_copy(
            src_ref=src,
            dst_ref=dst,
            send_sem=send.at[k],
            recv_sem=recv.at[k],
            device_id=peer,
            device_id_type=MESH,
        )
        made.start()
        started.append(made)
        return made

    def spread_out(k, peers, src, dst, whole):
        for peer in peers:
            pltpu.make_async_remote_copy(
                src_ref=src(peer),
                dst_ref=dst,
                send_sem=sum_send.at[k],
                recv_sem=sum_recv.at[k],
                device_id=peer,
                device_id_type=MESH,
            ).start()
        part = whole.at[pl.ds(0, len(peers))]
        return pltpu.make_async_remote_copy(
            src_ref=part,
            dst_ref=part,
            send_sem=sum_send.at[k],
            recv_sem=sum_recv.at[k],
            device_id=peers[0],
            device_id_type=MESH,
        )

    fetched[0].wait()
    fetched[1].wait()
    own = [
        copy(fr.at[1, half], fr.at[1, half], near[0]),
        copy(fr.at[2, half], fr.at[2, half], near[0]),
    ]
    below = [copy(fr.at[2, half], fr.at[0, half], near[3]), copy(fr.at[2, half], fr.at[0, half], near[4])]
    above = [copy(fr.at[1, half], fr.at[3, half], near[1]), copy(fr.at[1, half], fr.at[3, half], near[2])]

    clear_rows(x1, 8)
    clear_rows(x2, 4)
    clear_rows(g2c, 4)
    clear_rows(g1c, 8)
    fetched[2].wait()
    for a in range(3):
        w1f[a] = jnp.concatenate(
            [w1[9 * a + t, half, :].astype(F32) for t in range(9)], axis=1
        ).astype(BF16)

    lower = place > 0
    upper = place < total - 1

    def fill_one(p):
        turn[p] = fr[p].astype(F32).reshape(256, 128)
        for r in range(8):
            value = turn[p, pl.ds(r, 32, stride=8), :]
            if p == 0:
                value = jnp.where(lower, value, 0.0)
            if p == 3:
                value = jnp.where(upper, value, 0.0)
            fill_columns(x1, p, 32, r, value, True, False)

    own[0].wait_recv()
    fill_one(1)
    own[1].wait_recv()
    fill_one(2)
    pre = [
        dot(w1f[1], windows(x1, 1, 1024)) + dot(w1f[2], windows(x1, 2, 1024)),
        dot(w1f[0], windows(x1, 1, 1024)) + dot(w1f[1], windows(x1, 2, 1024)),
    ]

    fetched[3].wait()
    for a in range(3):
        w2b[a] = jnp.concatenate(
            [w2[9 * a + t, half, :].astype(F32) for t in range(9)], axis=1
        ).astype(BF16)
        turned[0:288, 0:64] = w2[9 * a : 9 * a + 9].astype(F32).reshape(288, 64)
        for b in range(3):
            block = jnp.transpose(turned[b * 128 : (b + 1) * 128, :])
            w2f[a, :, b * 128 : (b + 1) * 128] = block[0:64].astype(BF16)
        turned[0:288, 0:32] = w1[9 * a : 9 * a + 9].astype(F32).reshape(288, 32)
        for b in range(3):
            block = jnp.transpose(turned[b * 128 : (b + 1) * 128, :])
            w1b[a, :, b * 128 : (b + 1) * 128] = block[0:32].astype(BF16)
    fetched[4].wait()
    for c in range(32):
        turn[4, c * 8 : c * 8 + 4, 0:64] = cot[c, 0].astype(F32)
    lane = lax.broadcasted_iota(jnp.int32, (32, 128), 1)
    cots = [
        jnp.where(lane < 64, turn[4, pl.ds(r, 32, stride=8), :], 0.0) for r in range(4)
    ]
    cots = jnp.concatenate(cots, axis=1)

    for made in below:
        made.wait_recv()
    fill_one(0)
    pre[0] += dot(w1f[0], windows(x1, 0, 1024))
    for made in above:
        made.wait_recv()
    fill_one(3)
    pre[1] += dot(w1f[2], windows(x1, 3, 1024))

    act = []
    for plane in range(2):
        sig = jax.nn.sigmoid(pre[plane])
        s1[:, plane * 1024 : (plane + 1) * 1024] = slope_of(pre[plane], sig)
        act.append((pre[plane] * sig).astype(BF16))

    def act_row(plane, r):
        return act[plane][:, r * 128 : (r + 1) * 128]

    spots = jnp.concatenate(
        [
            jnp.concatenate(
                [act_row(a, 2 * r + b) for a in range(2) for b in range(2)], axis=1
            )
            for r in range(4)
        ],
        axis=0,
    )
    from_cell = lax.broadcasted_iota(jnp.int32, (512, 128), 0)
    to_cell = lax.broadcasted_iota(jnp.int32, (512, 128), 1)
    pool = jnp.where(((from_cell & 127) >> 1) == to_cell, 0.125, 0.0).astype(BF16)
    pooled = dot(spots, pool).astype(BF16).astype(F32)
    p2r[1, half] = pack_rows([pooled[16 * r : 16 * r + 16] for r in range(4)]).astype(BF16)

    def exchange(ref, part):
        below = [copy(ref.at[1, part], ref.at[0, part], near[3]), copy(ref.at[1, part], ref.at[0, part], near[4])]
        above = [copy(ref.at[1, part], ref.at[2, part], near[1]), copy(ref.at[1, part], ref.at[2, part], near[2])]
        own = copy(ref.at[1, part], ref.at[1, part], near[0])
        return own, below, above

    def fill_two(src, dst, chans, p, flip):
        packed = src[p].astype(F32)
        if p == 0:
            packed = jnp.where(lower, packed, 0.0)
        if p == 2:
            packed = jnp.where(upper, packed, 0.0)
        unpack_into(dst, p, chans, packed, flip)

    own, below, above = exchange(p2r, half)
    own.wait_recv()
    fill_two(p2r, x2, 32, 1, False)

    def part_two(a):
        return dot(w2f[a, half2, 0:288], windows(x2, a, 512))

    pre = part_two(1)
    for made in below:
        made.wait_recv()
    fill_two(p2r, x2, 32, 0, False)
    pre += part_two(0)
    for made in above:
        made.wait_recv()
    fill_two(p2r, x2, 32, 2, False)
    pre += part_two(2)
    sig = jax.nn.sigmoid(pre)
    grad = (cots * slope_of(pre, sig)).astype(BF16).astype(F32)
    g2r[1, half2] = pack_rows([grad[:, r * 128 : (r + 1) * 128] for r in range(4)]).astype(BF16)

    own, below, above = exchange(g2r, half2)
    own.wait_recv()
    fill_two(g2r, g2c, 64, 1, True)

    def part_back(a):
        return dot(w2b[a], windows(g2c, 2 - a, 512, True))

    back = part_back(1)
    sums = dot_rows(
        own_windows(x2, range(3), 512, core),
        jnp.concatenate([g2c[1, 64:128, 128:640], jnp.zeros((64, 512), BF16)], axis=0),
    )
    sums = jnp.concatenate([sums, jnp.zeros((16, 128), F32)], axis=0)
    sums = sums[0:224] + pltpu.roll(sums[224:448], 64, 1)
    size2 = 256 // flat
    for i in range(flat):
        if (i + 1) * size2 <= 224:
            ws2[i] = sums[i * size2 : (i + 1) * size2]
        else:
            ws2[i] = jnp.zeros((size2, 128), F32)
            if i * size2 < 224:
                ws2[i, 0 : 224 - i * size2] = sums[i * size2 : 224]
    for made in below:
        made.wait_recv()
    fill_two(g2r, g2c, 64, 0, True)
    back += part_back(2)
    for made in above:
        made.wait_recv()
    fill_two(g2r, g2c, 64, 2, True)
    back += part_back(0)

    def chunk(ref):
        return lambda peer: ref.at[peer[1] * nx + peer[2]]

    scatter2 = spread_out(0, across, chunk(ws2), rx2.at[mine], rx2)

    back = jnp.concatenate([back[:, r * 128 : (r + 1) * 128] for r in range(4)], axis=0)
    high = back.astype(BF16)
    rest = back - high.astype(F32)
    middle = rest.astype(BF16)
    low = (rest - middle.astype(F32)).astype(BF16)
    from_cell = lax.broadcasted_iota(jnp.int32, (128, 128), 0)
    to_cell = lax.broadcasted_iota(jnp.int32, (128, 128), 1)
    repeat = jnp.where(from_cell == (to_cell >> 1), 1.0, 0.0).astype(BF16)
    wide = dot(jnp.concatenate([high, middle, low], axis=0), repeat)
    wide = (wide[0:64] + wide[64:128] + wide[128:192]) * 0.125
    for plane in range(2):
        for r in range(8):
            first = plane * 1024 + r * 128
            value = wide[(r // 2) * 16 : (r // 2) * 16 + 16] * s1[:, first : first + 128]
            g1r[1 + plane, half, r * 128 : (r + 1) * 128] = value.astype(BF16)
    both = pl.ds(1, 2)
    own = copy(g1r.at[both, half], g1r.at[both, half], near[0])
    below = [copy(g1r.at[2, half], g1r.at[0, half], near[3]), copy(g1r.at[2, half], g1r.at[0, half], near[4])]
    above = [copy(g1r.at[1, half], g1r.at[3, half], near[1]), copy(g1r.at[1, half], g1r.at[3, half], near[2])]

    own.wait_recv()
    zero = jnp.zeros((96, 1024), BF16)
    sums = dot_rows(
        own_windows(x1, range(0, 3), 1024, core), jnp.concatenate([g1r[1], zero], axis=0)
    ) + dot_rows(
        own_windows(x1, range(1, 4), 1024, core), jnp.concatenate([g1r[2], zero], axis=0)
    )
    sums = jnp.concatenate([sums, jnp.zeros((16, 128), F32)], axis=0)
    sums = (
        sums[0:112]
        + pltpu.roll(sums[112:224], 32, 1)
        + pltpu.roll(sums[224:336], 64, 1)
        + pltpu.roll(sums[336:448], 96, 1)
    )
    size1 = 128 // flat
    for i in range(flat):
        if (i + 1) * size1 <= 112:
            ws1[i] = sums[i * size1 : (i + 1) * size1]
        else:
            ws1[i] = jnp.zeros((size1, 128), F32)
            if i * size1 < 112:
                ws1[i, 0 : 112 - i * size1] = sums[i * size1 : 112]
    scatter1 = spread_out(1, across, chunk(ws1), rx1.at[mine], rx1)

    def total_of(ref, n):
        parts = [ref[k] for k in range(n)]
        while len(parts) > 1:
            parts = [a + b for a, b in zip(parts[::2], parts[1::2])]
        return parts[0]

    def to_z(k, scatter, ws, rx, acc, rz):
        rx[mine] = ws[mine]
        scatter.wait_recv()
        part = total_of(rx, flat)
        acc[...] = part
        rz[z] = part
        return spread_out(k, along_z, lambda peer: acc, rz.at[z], rz)

    def to_all(k, meet, rz, fin):
        meet.wait_recv()
        fin[mine] = total_of(rz, nz)
        return spread_out(k, across, lambda peer: fin.at[mine], fin.at[mine], fin)

    meet2 = to_z(2, scatter2, ws2, rx2, acc2, rz2)

    def fill_grad(p):
        for r in range(8):
            value = g1r[p, :, r * 128 : (r + 1) * 128].astype(F32)
            if p == 0:
                value = jnp.where(lower, value, 0.0)
            if p == 3:
                value = jnp.where(upper, value, 0.0)
            fill_columns(g1c, p, 32, r, value, True, True)

    fill_grad(1)
    fill_grad(2)
    for made in below + above:
        made.wait_recv()
    fill_grad(0)
    fill_grad(3)
    for plane in range(2):
        grad = sum(
            dot(w1b[a, half, 0:288], windows(g1c, plane + 2 - a, 1024, True)) for a in range(3)
        )
        for r in range(8):
            turn[plane, pl.ds(r, 16, stride=8), :] = grad[:, r * 128 : (r + 1) * 128]
        gfv[:, plane] = turn[plane, 0:128].reshape(16, 8, 128).astype(BF16)
    stored = fetch(gfv, gf, 5)

    meet1 = to_z(3, scatter1, ws1, rx1, acc1, rz1)
    gather2 = to_all(4, meet2, rz2, fin2)
    gather1 = to_all(5, meet1, rz1, fin1)
    for made in started:
        made.wait_send()
    for made in (scatter1, scatter2, meet1, meet2):
        made.wait_send()
    stored.wait()
    gather2.wait()
    out2[...] = fin2[...]
    gather1.wait()
    out1[...] = fin1[...]


def finish(flat, gf, sum1, sum2, gf_out, gw1, gw2, all1, all2):
    gf_out[...] = gf[...]
    size1, size2 = 128 // flat, 256 // flat
    for i in range(flat):
        all1[i * size1 : (i + 1) * size1] = sum1[i]
        all2[i * size2 : (i + 1) * size2] = sum2[i]
    for j in range(4):
        rows = min(112, 432 - j * 112)
        part = all1[0:rows]
        part = pltpu.roll(part, 128 - 32 * j, 1) if j else part
        gw1[j * 112 : j * 112 + rows] = part[:, 0:32]
    gw2[0:224] = all2[0:224, 0:64]
    gw2[224:432] = pltpu.roll(all2[0:208], 64, 1)[:, 0:64]


def shards(sizes, feats, weight_one, weight_two, cotangent):
    nz, ny, nx = sizes
    flat = nx * ny
    w1 = jnp.transpose(weight_one, (2, 0, 1))
    w2 = jnp.transpose(weight_two, (2, 1, 0))
    vmem = pl.BlockSpec(memory_space=pltpu.VMEM)
    anywhere = pl.BlockSpec(memory_space=pl.ANY)
    copies = 6 + 5 + 5 + 5

    def scratch(rows):
        return [
            pltpu.VMEM((flat, rows // flat, 128), F32),
            pltpu.VMEM((flat, rows // flat, 128), F32),
            pltpu.VMEM((rows // flat, 128), F32),
            pltpu.VMEM((nz, rows // flat, 128), F32),
            pltpu.VMEM((flat, rows // flat, 128), F32),
        ]

    gf, sum1, sum2 = pl.pallas_call(
        functools.partial(kernel, sizes),
        out_shape=(
            jax.ShapeDtypeStruct((16, 2, 8, 128), BF16),
            jax.ShapeDtypeStruct((flat, 128 // flat, 128), F32),
            jax.ShapeDtypeStruct((flat, 256 // flat, 128), F32),
        ),
        in_specs=[anywhere] * 4,
        out_specs=(anywhere, vmem, vmem),
        scratch_shapes=[
            pltpu.VMEM((27, 32, 32), BF16),
            pltpu.VMEM((27, 32, 64), BF16),
            pltpu.VMEM((32, 1, 4, 64), BF16),
            pltpu.VMEM((3, 16, 288), BF16),
            pltpu.VMEM((3, 64, 384), BF16),
            pltpu.VMEM((3, 16, 576), BF16),
            pltpu.VMEM((3, 32, 384), BF16),
            pltpu.VMEM((384, 128), F32),
            pltpu.VMEM((4, 32, 8, 128), BF16),
            pltpu.VMEM((5, 256, 128), F32),
            pltpu.VMEM((4, 96, 1280), BF16),
            pltpu.VMEM((16, 2048), F32),
            pltpu.VMEM((3, 32, 256), BF16),
            pltpu.VMEM((3, 96, 768), BF16),
            pltpu.VMEM((3, 64, 256), BF16),
            pltpu.VMEM((3, 192, 768), BF16),
            pltpu.VMEM((4, 32, 1024), BF16),
            pltpu.VMEM((4, 96, 1280), BF16),
            pltpu.VMEM((16, 2, 8, 128), BF16),
            *scratch(128),
            *scratch(256),
            pltpu.SemaphoreType.DMA((6,)),
            pltpu.SemaphoreType.DMA((copies,)),
            pltpu.SemaphoreType.DMA((copies,)),
            pltpu.SemaphoreType.DMA((6,)),
            pltpu.SemaphoreType.DMA((6,)),
        ],
        compiler_params=pltpu.CompilerParams(
            collective_id=0, has_side_effects=True, vmem_limit_bytes=32 * 2**20
        ),
    )(feats, w1, w2, cotangent)
    gf, gw1, gw2 = pl.pallas_call(
        functools.partial(finish, flat),
        out_shape=(
            jax.ShapeDtypeStruct((16, 2, 8, 128), BF16),
            jax.ShapeDtypeStruct((432, 32), F32),
            jax.ShapeDtypeStruct((432, 64), F32),
        ),
        in_specs=[vmem] * 3,
        out_specs=(vmem, vmem, vmem),
        scratch_shapes=[pltpu.VMEM((128, 128), F32), pltpu.VMEM((256, 128), F32)],
        compiler_params=pltpu.CompilerParams(vmem_limit_bytes=8 * 2**20),
    )(gf, sum1, sum2)
    gw1 = jnp.transpose(gw1.reshape(27, 16, 32), (2, 1, 0))
    gw2 = jnp.transpose(gw2.reshape(27, 16, 64), (2, 1, 0))
    return gf, gw1, gw2


def build(mesh, sizes):
    finer = Mesh(mesh.devices.reshape(*sizes, mesh.shape["chan"]), AXES)
    depth = AXES[:3]
    in_specs = (P("core", depth, None, None), P(), P(), P("core", depth, None, None))
    out_specs = (P("core", depth, None, None), P(None, "core", None), P(None, "core", None))
    return jax.shard_map(
        functools.partial(shards, sizes),
        mesh=finer,
        in_specs=in_specs,
        out_specs=out_specs,
        check_vma=False,
    )


def solution(mesh):
    return build(mesh, (8, 8, 4))
```
